32 devices in a mesh: row: 4 (over z), col: 8 (over y, x, core).
Axes of the slice: x: 2, y: 2, z: 4, core: 2. Of those that a mesh axis runs over, the one named last changes fastest.
Arguments:
- minus_gradient: float32 [6, 16384], P(None, ('row', 'col')), may hold values from -10 to 10
- diag_blocks: float32 [36, 16384], P(None, ('row', 'col')), may hold values from -1000 to 1000, as said below
- hess_blocks: float32 [4, 8, 36, 4096], P('row', 'col'), may hold values from -40 to 40, as said below
- block_rows: int32 [4, 8, 4096], P('row', 'col'), may hold values from 0 to 2047
- block_cols: int32 [4, 8, 4096], P('row', 'col'), may hold values from 0 to 4095
- block_counts: int32 [4, 8], P('row', 'col'), may hold values from 0 to 4096, as said below
Outputs:
- pose_update: float32 [6, 16384], P(None, ('row', 'col'))
- residual: float32 [6, 16384], P(None, ('row', 'col'))
The draws below stay inside these ranges and needn't reach their ends.
Inputs may be any that keep to these rules, and one draw needn't show every extreme that they name: `hess_blocks`: the live blocks of all tiles together with diag_blocks form a symmetric positive definite matrix; no live block lies on the diagonal; the slots after the live ones hold arbitrary entries. `diag_blocks`: each 6x6 block is symmetric positive definite. The live slots of a tile are its first block_counts slots.
All inputs are finite; a program needn't handle non-finite values.
Results may differ from the reference program's by a relative error of at most 0.0003.
Values sent between devices are 32-bit elements; how exact they have to be, the bound alone decides.
A program may use at most 64 MiB of HBM per device.

```python
import jax
import jax.numpy as jnp
from jax import lax

POSE_DEV = 512
ITERS = 3
SLOTS = 4096
LOOPS = 16384
N_ROW = 4
N_COL = 8


damping = 0.5


def skewed_index(key, count, length):
    first_key, second_key = jax.random.split(key)
    factor_one = jax.random.randint(first_key, (count,), 0, length)
    factor_two = jax.random.randint(second_key, (count,), 1, length + 1)
    return factor_one * factor_two // length


def tile_ranks(tile_key):
    ordering = jnp.argsort(tile_key, stable=True)
    ordered = tile_key[ordering]
    first_pos = jnp.searchsorted(ordered, ordered, side='left').astype(jnp.int32)
    ranked = jnp.arange(tile_key.shape[0], dtype=jnp.int32) - first_pos
    return jnp.zeros_like(tile_key).at[ordering].set(ranked)


def build_graph(key):
    pose_count = POSE_DEV * N_ROW * N_COL
    group_size = POSE_DEV * N_COL
    devices = N_ROW * N_COL
    subkeys = jax.random.split(key, 14)
    col_order = jax.random.permutation(subkeys[0], N_COL).astype(jnp.int32)
    row_order = jax.random.permutation(subkeys[1], N_ROW).astype(jnp.int32)
    col_source = col_order[skewed_index(subkeys[2], LOOPS, N_COL)]
    row_source = jax.random.randint(subkeys[3], (LOOPS,), 0, N_ROW)
    row_target = row_order[skewed_index(subkeys[4], LOOPS, N_ROW)]
    col_target = jax.random.randint(subkeys[5], (LOOPS,), 0, N_COL)
    pose_source = (row_source * N_COL + col_source) * POSE_DEV + jax.random.randint(subkeys[6], (LOOPS,), 0, POSE_DEV)
    pose_target = (row_target * N_COL + col_target) * POSE_DEV + jax.random.randint(subkeys[7], (LOOPS,), 0, POSE_DEV)
    pose_target = jnp.where(pose_target == pose_source, (pose_target + 1) % pose_count, pose_target)
    chain_start = jnp.arange(pose_count - 1, dtype=jnp.int32)
    sources = jnp.concatenate([chain_start, pose_source.astype(jnp.int32)])
    targets = jnp.concatenate([chain_start + 1, pose_target.astype(jnp.int32)])
    edge_count = pose_count - 1 + LOOPS
    jacobian_left = jax.random.normal(subkeys[9], (edge_count, 6, 6)) * 6.0 ** (-0.5)
    jacobian_right = jax.random.normal(subkeys[10], (edge_count, 6, 6)) * 6.0 ** (-0.5)
    off_forward = jnp.einsum('eki,ekj->eij', jacobian_left, jacobian_right).reshape(edge_count, 36)
    off_backward = jnp.einsum('eki,ekj->eij', jacobian_right, jacobian_left).reshape(edge_count, 36)
    all_rows = jnp.concatenate([sources, targets])
    all_cols = jnp.concatenate([targets, sources])
    values = jnp.concatenate([off_forward, off_backward])
    seg_rows = all_rows // POSE_DEV
    seg_cols = all_cols // POSE_DEV
    tile_row = seg_cols // N_COL
    tile_col = seg_rows % N_COL
    tile_ids = tile_row * N_COL + tile_col
    local_row = seg_rows // N_COL * POSE_DEV + all_rows % POSE_DEV
    local_col = all_cols - tile_row * group_size
    first_rank = tile_ranks(tile_ids)
    overflow = first_rank >= SLOTS
    keep_edge = jnp.logical_not(jnp.logical_or(overflow[:edge_count], overflow[edge_count:]))
    keep_all = jnp.concatenate([keep_edge, keep_edge])
    second_rank = tile_ranks(jnp.where(keep_all, tile_ids, devices))
    target_slot = jnp.where(keep_all, tile_ids * SLOTS + second_rank, devices * SLOTS)
    pad_rows = jax.random.randint(subkeys[11], (devices * SLOTS,), 0, N_ROW * POSE_DEV)
    pad_cols = jax.random.randint(subkeys[12], (devices * SLOTS,), 0, group_size)
    rows_out = pad_rows.at[target_slot].set(local_row, mode='drop').reshape(N_ROW, N_COL, SLOTS)
    cols_out = pad_cols.at[target_slot].set(local_col, mode='drop').reshape(N_ROW, N_COL, SLOTS)
    pad_values = jnp.clip(jax.random.normal(subkeys[13], (devices * SLOTS, 36)), -3.0, 3.0) * 0.5
    hess_out = pad_values.at[target_slot].set(values, mode='drop').reshape(N_ROW, N_COL, SLOTS, 36)
    hess_out = jnp.transpose(hess_out, (0, 1, 3, 2))
    counts_out = jax.ops.segment_sum(keep_all.astype(jnp.int32), tile_ids, num_segments=devices).reshape(N_ROW, N_COL)
    keep_float = keep_edge.astype(jnp.float32)[:, None]
    own_left = jnp.einsum('eki,ekj->eij', jacobian_left, jacobian_left).reshape(edge_count, 36) * keep_float
    own_right = jnp.einsum('eki,ekj->eij', jacobian_right, jacobian_right).reshape(edge_count, 36) * keep_float
    diagonal = jax.ops.segment_sum(own_left, sources, num_segments=pose_count)
    diagonal = diagonal + jax.ops.segment_sum(own_right, targets, num_segments=pose_count)
    diagonal = diagonal + damping * jnp.eye(6, dtype=jnp.float32).reshape(1, 36)
    return (hess_out, rows_out, cols_out, counts_out, jnp.transpose(diagonal))


def draw_hess_blocks(key, part):
    return build_graph(jax.random.fold_in(key, 11))[0]


def draw_block_rows(key, part):
    return build_graph(jax.random.fold_in(key, 11))[1]


def draw_block_cols(key, part):
    return build_graph(jax.random.fold_in(key, 11))[2]


def draw_block_counts(key, part):
    return build_graph(jax.random.fold_in(key, 11))[3]


def draw_diag_blocks(key, part):
    return build_graph(jax.random.fold_in(key, 11))[4]


def draw_minus_gradient(key, part):
    pose_count = POSE_DEV * N_ROW * N_COL
    scale_ramp = 0.5 + jnp.arange(pose_count, dtype=jnp.float32) / pose_count
    values = jnp.clip(jax.random.normal(key, (6, pose_count)), -6.0, 6.0) * scale_ramp
    return values


def setup_inputs(seed: int = 0) -> dict:
    keys = jax.random.split(jax.random.key(seed), 7)
    return {
        "minus_gradient": draw_minus_gradient(jax.random.fold_in(keys[6], 71), 0),
        "diag_blocks": draw_diag_blocks(jax.random.fold_in(keys[6], 71), 0),
        "hess_blocks": draw_hess_blocks(jax.random.fold_in(keys[6], 71), 0),
        "block_rows": draw_block_rows(jax.random.fold_in(keys[6], 71), 0),
        "block_cols": draw_block_cols(jax.random.fold_in(keys[6], 71), 0),
        "block_counts": draw_block_counts(jax.random.fold_in(keys[6], 71), 0),
    }


def factor_blocks(blocks):
    lower_part = {}
    reciprocals = []
    for j in range(6):
        pivot_value = blocks[7 * j]
        for k in range(j):
            pivot_value = pivot_value - lower_part[j, k] * lower_part[j, k]
        reciprocal = 1.0 / jnp.sqrt(pivot_value)
        reciprocals.append(reciprocal)
        for i in range(j + 1, 6):
            entry_value = blocks[6 * i + j]
            for k in range(j):
                entry_value = entry_value - lower_part[i, k] * lower_part[j, k]
            lower_part[i, j] = entry_value * reciprocal
    return (lower_part, reciprocals)

def apply_inverse(lower_part, reciprocals, vector):
    forward = []
    for i in range(6):
        running = vector[i]
        for k in range(i):
            running = running - lower_part[i, k] * forward[k]
        forward.append(running * reciprocals[i])
    backward = [None] * 6
    for i in range(5, -1, -1):
        running = forward[i]
        for k in range(i + 1, 6):
            running = running - lower_part[k, i] * backward[k]
        backward[i] = running * reciprocals[i]
    return jnp.stack(backward)

def diagonal_term(diag_blocks, vector):
    return lax.optimization_barrier(jnp.sum(diag_blocks.reshape(6, 6, -1) * vector[None], axis=1))

def apply_hessian(vector, diag_blocks, hess_blocks, block_rows, block_cols, block_counts):
    group_size = POSE_DEV * N_COL
    slot_ids = jnp.arange(SLOTS, dtype=jnp.int32)
    col_ids = jnp.arange(N_COL, dtype=jnp.int32)[:, None]

    def one_row(summed, r):
        blocks = hess_blocks[r].reshape(N_COL, 6, 6, SLOTS)
        local_rows = block_rows[r]
        global_rows = (local_rows // POSE_DEV * N_COL + col_ids) * POSE_DEV + local_rows % POSE_DEV
        global_cols = r * group_size + block_cols[r]
        live_mask = slot_ids[None, :] < block_counts[r][:, None]
        picked = jnp.take(vector, global_cols.reshape(-1), axis=1).reshape(6, N_COL, SLOTS)
        product = lax.optimization_barrier(jnp.sum(blocks * jnp.transpose(picked, (1, 0, 2))[:, None], axis=2))
        product = jnp.where(live_mask[:, None, :], product, 0.0)
        summed = summed.at[:, global_rows.reshape(-1)].add(jnp.transpose(product, (1, 0, 2)).reshape(6, -1))
        return (summed, None)
    summed, unused = lax.scan(one_row, jnp.zeros_like(vector), jnp.arange(N_ROW, dtype=jnp.int32))
    return summed + diagonal_term(diag_blocks, vector)

def reference(minus_gradient, diag_blocks, hess_blocks, block_rows, block_cols, block_counts):
    lower_part, reciprocals = factor_blocks(diag_blocks)

    def hessian(vector):
        return apply_hessian(vector, diag_blocks, hess_blocks, block_rows, block_cols, block_counts)
    solution = jnp.zeros_like(minus_gradient)
    residual = minus_gradient
    precond = apply_inverse(lower_part, reciprocals, residual)
    direction = precond
    rho_now = jnp.sum(residual * precond)
    for k in range(ITERS):
        hess_image = hessian(direction)
        step_size = rho_now / jnp.sum(direction * hess_image)
        solution = solution + step_size * direction
        residual = residual - step_size * hess_image
        if k + 1 < ITERS:
            precond = apply_inverse(lower_part, reciprocals, residual)
            rho_next = jnp.sum(residual * precond)
            direction = precond + rho_next / rho_now * direction
            rho_now = rho_next
    return (solution, residual)
```

```python
import functools

import jax
import jax.numpy as jnp
from jax import lax
from jax.experimental import pallas as pl
from jax.experimental.pallas import tpu as pltpu
from jax.sharding import PartitionSpec as P

ITERS = 3
LANES = 128
SUB = 8
MESH = pl.DeviceIdType.MESH


def xor_index(a, b, n):
    out = 0
    bit = 1
    while bit < n:
        out = out + bit * ((a // bit + b // bit) % 2)
        bit *= 2
    return out


def factor_blocks(entry):
    lower_part = {}
    reciprocals = []
    for j in range(6):
        pivot_value = entry(7 * j)
        for k in range(j):
            pivot_value = pivot_value - lower_part[j, k] * lower_part[j, k]
        reciprocal = 1.0 / jnp.sqrt(pivot_value)
        reciprocals.append(reciprocal)
        for i in range(j + 1, 6):
            entry_value = entry(6 * i + j)
            for k in range(j):
                entry_value = entry_value - lower_part[i, k] * lower_part[j, k]
            lower_part[i, j] = entry_value * reciprocal
    return lower_part, reciprocals


def apply_inverse(lower, recip, vector):
    forward = []
    for i in range(6):
        running = vector[i]
        for k in range(i):
            running = running - lower(i, k) * forward[k]
        forward.append(running * recip(i))
    backward = [None] * 6
    for i in range(5, -1, -1):
        running = forward[i]
        for k in range(i + 1, 6):
            running = running - lower(k, i) * backward[k]
        backward[i] = running * recip(i)
    return backward


def cg_scalars(m):
    rc, pc = [1.0], [1.0]
    xc = [0.0] * ITERS
    rho = m[0]
    for k in range(ITERS):
        hc = [0.0] * (k + 2)
        for i in range(k + 1):
            hc[i] = hc[i] + pc[i]
            hc[i + 1] = hc[i + 1] - pc[i]
        curv = 0.0
        for i in range(k + 1):
            for j in range(k + 2):
                curv = curv + pc[i] * hc[j] * m[i + j]
        step = rho / curv
        for i in range(k + 1):
            xc[i] = xc[i] + step * pc[i]
        rc = [a - step * b for a, b in zip(rc + [0.0], hc)]
        if k + 1 < ITERS:
            rho_next = 0.0
            for i in range(k + 2):
                for j in range(k + 2):
                    rho_next = rho_next + rc[i] * rc[j] * m[i + j]
            ratio = rho_next / rho
            pc = [a + ratio * b for a, b in zip(rc, pc + [0.0])]
            rho = rho_next
    return xc, rc


def kernel(
    nrow, ncol, cnt_ref, g_ref, d_ref, rows_ref, cols_ref, h_any, x_ref, r_ref,
    hbuf, b3, dbuf, lbuf, rv, vv, tab, vrow, tbuf, spread, onehot, part, rbuf, mom, mown,
    hsem, vs_sem, vr_sem, ws_sem, wr_sem, ps_sem, pr_sem, ms_sem, mr_sem,
):
    pose_dev = g_ref.shape[1]
    qn = pose_dev // LANES
    vec = 6 * qn
    nchunk = rows_ref.shape[0]
    stride = nchunk + SUB
    nj = nchunk // SUB
    msg = part.shape[2]
    per = SUB // qn
    pairs = 6 // per
    my_row = lax.axis_index("row")
    my_col = lax.axis_index("col")

    h_copy = pltpu.make_async_copy(h_any, hbuf, hsem)
    h_copy.start()

    barrier = pltpu.get_barrier_semaphore()
    for i in range(1, ncol):
        pl.semaphore_signal(
            barrier, inc=1, device_id=(my_row, xor_index(my_col, i, ncol)), device_id_type=MESH
        )
    for i in range(1, nrow):
        pl.semaphore_signal(
            barrier, inc=1, device_id=(xor_index(my_row, i, nrow), my_col), device_id_type=MESH
        )

    for b in range(6):
        for q in range(qn):
            rv[0, b * qn + q : b * qn + q + 1, :] = g_ref[b : b + 1, q * LANES : (q + 1) * LANES]
    for e in range(0, 36, SUB):
        count = min(SUB, 36 - e)
        for q in range(qn):
            dbuf[pl.ds(e * qn + q, count, stride=qn), :] = d_ref[
                e : e + count, q * LANES : (q + 1) * LANES
            ]

    def diag(e):
        return dbuf[e * qn : (e + 1) * qn, :]

    lower_part, reciprocals = factor_blocks(diag)
    slot_of = {}
    for n, (key, value) in enumerate(list(lower_part.items()) + list(enumerate(reciprocals))):
        slot_of[key] = n
        lbuf[n] = value

    def lower(i, k):
        return lbuf[slot_of[i, k]]

    def recip(i):
        return lbuf[slot_of[i]]

    def precondition(k):
        out = apply_inverse(lower, recip, [rv[k, b * qn : (b + 1) * qn, :] for b in range(6)])
        for b in range(6):
            vv[k, b * qn : (b + 1) * qn, :] = out[b]

    def send_vector(k):
        copies = []
        for i in range(1, ncol):
            copy = pltpu.make_async_remote_copy(
                src_ref=vv.at[k],
                dst_ref=tab.at[k, my_col],
                send_sem=vs_sem.at[k, i],
                recv_sem=vr_sem.at[k, i],
                device_id=(my_row, xor_index(my_col, i, ncol)),
                device_id_type=MESH,
            )
            copy.start()
            copies.append(copy)
        return copies

    def send_rows(k):
        copies = []
        for i in range(1, nrow):
            copy = pltpu.make_async_remote_copy(
                src_ref=vv.at[k],
                dst_ref=vrow.at[my_row],
                send_sem=ws_sem.at[i],
                recv_sem=wr_sem.at[i],
                device_id=(xor_index(my_row, i, nrow), my_col),
                device_id_type=MESH,
            )
            copy.start()
            copies.append(copy)
        return copies

    precondition(0)
    pl.semaphore_wait(barrier, ncol + nrow - 2)
    sends = send_vector(0)

    sub_low = lax.broadcasted_iota(jnp.int32, (LANES, LANES), 0)

    def build_onehot(j, carry):
        low = rows_ref[pl.ds(pl.multiple_of(j * SUB, SUB), SUB), :] % LANES
        for s in range(SUB):
            hot = jnp.where(sub_low == low[s : s + 1, :], 1.0, 0.0).astype(jnp.bfloat16)
            onehot[:, pl.ds(pl.multiple_of((j * SUB + s) * LANES, LANES), LANES)] = hot
        return carry

    lax.fori_loop(0, nj, build_onehot, 0)

    h_copy.wait()
    live_count = cnt_ref[0, 0]
    lane = lax.broadcasted_iota(jnp.int32, (SUB, LANES), 1)
    for c in range(nchunk):
        live = lane + c * LANES < live_count
        for e in range(0, 36, SUB):
            count = min(SUB, 36 - e)
            tile = hbuf[e : e + count, c * LANES : (c + 1) * LANES]
            b3[pl.ds(e * stride + c, count, stride=stride), :] = jnp.where(
                live[:count], tile, 0.0
            )

    sub = lax.broadcasted_iota(jnp.int32, (SUB, LANES), 0)
    sub_q = sub % qn
    sub_b = sub // qn

    def tile_partial(k):
        low = [cols_ref[j * SUB : (j + 1) * SUB, :] % LANES for j in range(nj)]
        high = [cols_ref[j * SUB : (j + 1) * SUB, :] // LANES for j in range(nj)]

        def pick(dev, source, acc):
            acc = list(acc)
            for q in range(qn):
                for j in range(nj):
                    chosen = high[j] == dev * qn + q
                    for b in range(6):
                        row = jnp.broadcast_to(source(b * qn + q), (SUB, LANES))
                        got = jnp.take_along_axis(row, low[j], axis=1)
                        acc[b * nj + j] = jnp.where(chosen, got, acc[b * nj + j])
            return tuple(acc)

        zero = tuple(jnp.zeros((SUB, LANES), jnp.float32) for _ in range(6 * nj))
        acc = pick(my_col, lambda n: vv[k, n : n + 1, :], zero)

        def one_peer(i, acc):
            peer = xor_index(my_col, i, ncol)
            pltpu.make_async_remote_copy(
                src_ref=vv.at[k],
                dst_ref=tab.at[k, peer],
                send_sem=vs_sem.at[k, i],
                recv_sem=vr_sem.at[k, i],
                device_id=(my_row, peer),
                device_id_type=MESH,
            ).wait_recv()
            return pick(peer, lambda n: tab[k, peer, n : n + 1, :], acc)

        acc = lax.fori_loop(1, ncol, one_peer, acc)
        for a in range(6):
            for j in range(nj):
                term = None
                for b in range(6):
                    start = (6 * a + b) * stride + j * SUB
                    product = b3[start : start + SUB, :] * acc[b * nj + j]
                    term = product if term is None else term + product
                tbuf[a * nchunk + j * SUB : a * nchunk + (j + 1) * SUB, :] = term

        def spread_group(j, carry):
            base = pl.multiple_of(j * SUB, SUB)
            row_high = rows_ref[pl.ds(base, SUB), :] // LANES
            terms = [tbuf[pl.ds(a * nchunk + base, SUB), :] for a in range(6)]
            for s in range(SUB):
                here = row_high[s : s + 1, :] - sub_q
                stacked = []
                for p in range(pairs):
                    value = jnp.broadcast_to(terms[p * per][s : s + 1, :], (SUB, LANES))
                    for o in range(1, per):
                        value = jnp.where(sub_b == o, terms[p * per + o][s : s + 1, :], value)
                    stacked.append(value)
                rows = []
                for d in range(nrow):
                    chosen = here == d * qn
                    for p in range(pairs):
                        rows.append(jnp.where(chosen, stacked[p], 0.0))
                full = jnp.concatenate(rows, axis=0)
                upper = full.astype(jnp.bfloat16)
                rest = (full - upper.astype(jnp.float32)).astype(jnp.bfloat16)
                where = pl.ds(pl.multiple_of((j * SUB + s) * LANES, LANES), LANES)
                spread[0 : nrow * vec, where] = upper
                spread[nrow * vec : 2 * nrow * vec, where] = rest
            return carry

        lax.fori_loop(0, nj, spread_group, 0)
        both = lax.dot_general(
            spread[...], onehot[...], (((1,), (1,)), ((), ())),
            preferred_element_type=jnp.float32,
        )
        total = both[: nrow * vec] + both[nrow * vec :]
        for d in range(nrow):
            part[k, d, 0:vec, :] = total[d * vec : (d + 1) * vec]

    def send_parts(k):
        size = msg if k == ITERS - 1 else vec
        copies = []
        for i in range(1, nrow):
            peer = xor_index(my_row, i, nrow)
            copy = pltpu.make_async_remote_copy(
                src_ref=part.at[k, peer, pl.ds(0, size)],
                dst_ref=rbuf.at[k, my_row, pl.ds(0, size)],
                send_sem=ps_sem.at[k, i],
                recv_sem=pr_sem.at[k, i],
                device_id=(peer, my_col),
                device_id_type=MESH,
            )
            copy.start()
            copies.append(copy)
        return copies

    def diag_image(k):
        out = []
        v = [vv[k, b * qn : (b + 1) * qn, :] for b in range(6)]
        for a in range(6):
            value = diag(6 * a) * v[0]
            for b in range(1, 6):
                value = value + diag(6 * a + b) * v[b]
            out.append(value)
        return out

    def row_sum(value):
        return jnp.sum(value, axis=0, keepdims=True)

    moments = [row_sum(vv[0] * rv[0])]
    for k in range(ITERS):
        own = diag_image(k)
        for a in range(6):
            rv[k + 1, a * qn : (a + 1) * qn, :] = rv[k, a * qn : (a + 1) * qn, :] - own[a]
        if k == ITERS - 1:
            curv = row_sum(vv[k] * (rv[k] - rv[k + 1]))
        tile_partial(k)
        if k == ITERS - 1:
            curv = curv + row_sum(vv[k] * part[k, my_row, 0:vec, :])
            for i in range(1, nrow):
                peer = xor_index(my_row, i, nrow)
                row_copies[i - 1].wait_recv()
                curv = curv + row_sum(vrow[peer] * part[k, peer, 0:vec, :])
            moments.append(curv)
            packed = jnp.zeros((SUB, LANES), jnp.float32)
            for n, value in enumerate(moments):
                packed = jnp.where(lane == n, jnp.sum(value, axis=1, keepdims=True), packed)
            for d in range(nrow):
                part[k, d, vec:msg, :] = packed
        sent = send_parts(k)
        image = part[k, my_row, 0:vec, :]
        for i in range(1, nrow):
            sent[i - 1].wait_recv()
            peer = xor_index(my_row, i, nrow)
            image = image + rbuf[k, peer, 0:vec, :]
            if k == ITERS - 1:
                packed = packed + rbuf[k, peer, vec:msg, :]
        sends += sent
        if k == ITERS - 1:
            mown[...] = packed
            total_m = packed
            mom_sends = []
            for i in range(1, ncol):
                copy = pltpu.make_async_remote_copy(
                    src_ref=mown,
                    dst_ref=mom.at[my_col],
                    send_sem=ms_sem.at[i],
                    recv_sem=mr_sem.at[i],
                    device_id=(my_row, xor_index(my_col, i, ncol)),
                    device_id_type=MESH,
                )
                copy.start()
                mom_sends.append(copy)
        rv[k + 1] = rv[k + 1] - image
        if k + 1 < ITERS:
            precondition(k + 1)
            sends += send_vector(k + 1)
            if k + 1 == ITERS - 1:
                row_copies = send_rows(k + 1)
            moments.append(row_sum(vv[k] * rv[k + 1]))
            moments.append(row_sum(vv[k + 1] * rv[k + 1]))

    for i in range(1, ncol):
        mom_sends[i - 1].wait_recv()
        total_m = total_m + mom[xor_index(my_col, i, ncol)]
    m = [
        jnp.broadcast_to(
            jnp.sum(jnp.where(lane == n, total_m, 0.0), axis=1, keepdims=True), (SUB, LANES)
        )
        for n in range(2 * ITERS)
    ]
    m[2 * ITERS - 1] = m[2 * ITERS - 2] - m[2 * ITERS - 1]
    xc, rc = cg_scalars(m)
    for b in range(6):
        for q in range(qn):
            n = b * qn + q
            x = None
            r = None
            for k in range(ITERS + 1):
                add = rc[k][0:1] * rv[k, n : n + 1, :]
                r = add if r is None else r + add
                if k < ITERS:
                    add = xc[k][0:1] * vv[k, n : n + 1, :]
                    x = add if x is None else x + add
            x_ref[b : b + 1, q * LANES : (q + 1) * LANES] = x
            r_ref[b : b + 1, q * LANES : (q + 1) * LANES] = r
    for copy in sends + row_copies + mom_sends:
        copy.wait_send()


def on_device(nrow, ncol, minus_gradient, diag_blocks, hess_blocks, block_rows, block_cols, counts):
    pose_dev = minus_gradient.shape[1]
    nslot = block_rows.shape[-1]
    nchunk = nslot // LANES
    vec = 6 * pose_dev // LANES
    msg = vec + SUB
    f32 = jnp.float32
    vmem = pl.BlockSpec(memory_space=pltpu.VMEM)
    dma = pltpu.SemaphoreType.DMA
    out = jax.ShapeDtypeStruct(minus_gradient.shape, f32)
    return pl.pallas_call(
        functools.partial(kernel, nrow, ncol),
        out_shape=(out, out),
        in_specs=[
            pl.BlockSpec(memory_space=pltpu.SMEM), vmem, vmem, vmem, vmem,
            pl.BlockSpec(memory_space=pl.ANY),
        ],
        out_specs=(vmem, vmem),
        scratch_shapes=[
            pltpu.VMEM((36, nslot), f32),
            pltpu.VMEM((36 * (nchunk + SUB), LANES), f32),
            pltpu.VMEM((6 * vec, LANES), f32),
            pltpu.VMEM((21, pose_dev // LANES, LANES), f32),
            pltpu.VMEM((ITERS + 1, vec, LANES), f32),
            pltpu.VMEM((ITERS, vec, LANES), f32),
            pltpu.VMEM((ITERS, ncol, vec, LANES), f32),
            pltpu.VMEM((nrow, vec, LANES), f32),
            pltpu.VMEM((6 * nchunk, LANES), f32),
            pltpu.VMEM((2 * nrow * vec, nslot), jnp.bfloat16),
            pltpu.VMEM((LANES, nslot), jnp.bfloat16),
            pltpu.VMEM((ITERS, nrow, msg, LANES), f32),
            pltpu.VMEM((ITERS, nrow, msg, LANES), f32),
            pltpu.VMEM((ncol, SUB, LANES), f32),
            pltpu.VMEM((SUB, LANES), f32),
            dma,
            dma((ITERS, ncol)), dma((ITERS, ncol)),
            dma((nrow,)), dma((nrow,)),
            dma((ITERS, nrow)), dma((ITERS, nrow)),
            dma((ncol,)), dma((ncol,)),
        ],
        compiler_params=pltpu.CompilerParams(
            collective_id=0, has_side_effects=True, vmem_limit_bytes=48 * 1024 * 1024
        ),
    )(
        counts,
        minus_gradient,
        diag_blocks,
        block_rows.reshape(nchunk, LANES),
        block_cols.reshape(nchunk, LANES),
        hess_blocks.reshape(36, nslot),
    )


def solution(mesh):
    placed = (
        P(None, ("row", "col")),
        P(None, ("row", "col")),
        P("row", "col", None, None),
        P("row", "col", None),
        P("row", "col", None),
        P("row", "col"),
    )
    return jax.shard_map(
        functools.partial(on_device, mesh.shape["row"], mesh.shape["col"]),
        mesh=mesh,
        in_specs=placed,
        out_specs=(P(None, ("row", "col")), P(None, ("row", "col"))),
        check_vma=False,
    )
```

```python
import functools

import jax
import jax.numpy as jnp
from jax import lax
from jax.experimental import pallas as pl
from jax.experimental.pallas import tpu as pltpu
from jax.sharding import PartitionSpec as P

ITERS = 3
LANES = 128
SUB = 8
MESH = pl.DeviceIdType.MESH


def xor_index(a, b, n):
    out = 0
    bit = 1
    while bit < n:
        out = out + bit * ((a // bit + b // bit) % 2)
        bit *= 2
    return out


def split_index(value, size):
    if size & (size - 1) == 0:
        return value >> (size.bit_length() - 1), value & (size - 1)
    return lax.div(value, size), lax.rem(value, size)


def factor_blocks(entry):
    lower_part = {}
    reciprocals = []
    for j in range(6):
        pivot_value = entry(7 * j)
        for k in range(j):
            pivot_value = pivot_value - lower_part[j, k] * lower_part[j, k]
        reciprocal = 1.0 / jnp.sqrt(pivot_value)
        reciprocals.append(reciprocal)
        for i in range(j + 1, 6):
            entry_value = entry(6 * i + j)
            for k in range(j):
                entry_value = entry_value - lower_part[i, k] * lower_part[j, k]
            lower_part[i, j] = entry_value * reciprocal
    return lower_part, reciprocals


def apply_inverse(lower, recip, vector):
    forward = []
    for i in range(6):
        running = vector[i]
        for k in range(i):
            running = running - lower(i, k) * forward[k]
        forward.append(running * recip(i))
    backward = [None] * 6
    for i in range(5, -1, -1):
        running = forward[i]
        for k in range(i + 1, 6):
            running = running - lower(k, i) * backward[k]
        backward[i] = running * recip(i)
    return backward


def cg_scalars(m):
    rc, pc = [1.0], [1.0]
    xc = [0.0] * ITERS
    rho = m[0]
    for k in range(ITERS):
        hc = [0.0] * (k + 2)
        for i in range(k + 1):
            hc[i] = hc[i] + pc[i]
            hc[i + 1] = hc[i + 1] - pc[i]
        curv = 0.0
        for i in range(k + 1):
            for j in range(k + 2):
                curv = curv + pc[i] * hc[j] * m[i + j]
        step = rho / curv
        for i in range(k + 1):
            xc[i] = xc[i] + step * pc[i]
        rc = [a - step * b for a, b in zip(rc + [0.0], hc)]
        if k + 1 < ITERS:
            rho_next = 0.0
            for i in range(k + 2):
                for j in range(k + 2):
                    rho_next = rho_next + rc[i] * rc[j] * m[i + j]
            ratio = rho_next / rho
            pc = [a + ratio * b for a, b in zip(rc, pc + [0.0])]
            rho = rho_next
    return xc, rc


def kernel(
    nrow, ncol, cnt_any, g_any, d_any, rows_any, cols_any, h_any, x_ref, r_ref,
    cnt_ref, g_ref, d_ref, rows_ref, cols_ref, b3, dbuf, lbuf, rv, vv, tab, vrow, key, tbuf, spread, onehot, part, rbuf, mom, mown,
    in_sem, vs_sem, vr_sem, ws_sem, wr_sem, ps_sem, pr_sem, ms_sem, mr_sem,
):
    pose_dev = g_ref.shape[1]
    qn = pose_dev // LANES
    vec = 6 * qn
    nchunk = rows_ref.shape[0]
    nj = nchunk // SUB
    msg = part.shape[2]
    per = SUB // qn
    pairs = 6 // per
    my_row = lax.axis_index("row")
    my_col = lax.axis_index("col")

    loads = [
        pltpu.make_async_copy(source, target, in_sem.at[n])
        for n, (source, target) in enumerate(
            [
                (d_any, d_ref), (g_any, g_ref), (rows_any, rows_ref),
                (cols_any, cols_ref), (h_any, b3), (cnt_any, cnt_ref),
            ]
        )
    ]
    for load in loads:
        load.start()

    barrier = pltpu.get_barrier_semaphore()
    for i in range(1, ncol):
        pl.semaphore_signal(
            barrier, inc=1, device_id=(my_row, xor_index(my_col, i, ncol)), device_id_type=MESH
        )
    for i in range(1, nrow):
        pl.semaphore_signal(
            barrier, inc=1, device_id=(xor_index(my_row, i, nrow), my_col), device_id_type=MESH
        )

    loads[0].wait()
    loads[1].wait()
    for b in range(6):
        for q in range(qn):
            rv[0, b * qn + q : b * qn + q + 1, :] = g_ref[b : b + 1, q * LANES : (q + 1) * LANES]
    for e in range(0, 36, SUB):
        count = min(SUB, 36 - e)
        for q in range(qn):
            dbuf[pl.ds(e * qn + q, count, stride=qn), :] = d_ref[
                e : e + count, q * LANES : (q + 1) * LANES
            ]

    def diag(e):
        return dbuf[e * qn : (e + 1) * qn, :]

    lower_part, reciprocals = factor_blocks(diag)
    slot_of = {}
    for n, (name, value) in enumerate(list(lower_part.items()) + list(enumerate(reciprocals))):
        slot_of[name] = n
        lbuf[n] = value

    def lower(i, k):
        return lbuf[slot_of[i, k]]

    def recip(i):
        return lbuf[slot_of[i]]

    def precondition(k):
        out = apply_inverse(lower, recip, [rv[k, b * qn : (b + 1) * qn, :] for b in range(6)])
        for b in range(6):
            vv[k, b * qn : (b + 1) * qn, :] = out[b]

    def send_vector(k):
        copies = []
        for i in range(1, ncol):
            copy = pltpu.make_async_remote_copy(
                src_ref=vv.at[k],
                dst_ref=tab.at[k, my_col],
                send_sem=vs_sem.at[k, i],
                recv_sem=vr_sem.at[k, i],
                device_id=(my_row, xor_index(my_col, i, ncol)),
                device_id_type=MESH,
            )
            copy.start()
            copies.append(copy)
        return copies

    def send_rows(k):
        copies = []
        for i in range(1, nrow):
            copy = pltpu.make_async_remote_copy(
                src_ref=vv.at[k],
                dst_ref=vrow.at[my_row],
                send_sem=ws_sem.at[i],
                recv_sem=wr_sem.at[i],
                device_id=(xor_index(my_row, i, nrow), my_col),
                device_id_type=MESH,
            )
            copy.start()
            copies.append(copy)
        return copies

    precondition(0)
    pl.semaphore_wait(barrier, ncol + nrow - 2)
    sends = send_vector(0)

    wide = 2 * LANES
    hot_row = lax.broadcasted_iota(jnp.int32, (wide, LANES), 0)

    def build_onehot(j, carry):
        row = rows_ref[pl.ds(pl.multiple_of(j * SUB, SUB), SUB), :]
        chunk, low = split_index(row, LANES)
        group, q = split_index(chunk, qn)
        group_half, parity = split_index(group, 2)
        key[pl.ds(pl.multiple_of(j * SUB, SUB), SUB), :] = group_half * qn + q
        target = parity * LANES + low
        for s in range(SUB):
            hot = jnp.where(hot_row == target[s : s + 1, :], 1.0, 0.0).astype(jnp.bfloat16)
            onehot[:, pl.ds(pl.multiple_of((j * SUB + s) * LANES, LANES), LANES)] = hot
        return carry

    loads[2].wait()
    lax.fori_loop(0, nj, build_onehot, 0)

    loads[3].wait()
    loads[4].wait()
    loads[5].wait()
    live_count = cnt_ref[0, 0]
    lane = lax.broadcasted_iota(jnp.int32, (SUB, LANES), 1)
    sub = lax.broadcasted_iota(jnp.int32, (SUB, LANES), 0)
    sub_q = sub % qn
    sub_b = sub // qn
    slot_id = sub * LANES + lane

    def tile_partial(k):
        split = [split_index(cols_ref[j * SUB : (j + 1) * SUB, :], LANES) for j in range(nj)]
        high = [pair[0] for pair in split]
        low = [pair[1] for pair in split]

        def pick(dev, source, acc):
            acc = list(acc)
            for q in range(qn):
                for j in range(nj):
                    chosen = high[j] == dev * qn + q
                    for b in range(6):
                        row = jnp.broadcast_to(source(b * qn + q), (SUB, LANES))
                        got = jnp.take_along_axis(row, low[j], axis=1)
                        acc[b * nj + j] = jnp.where(chosen, got, acc[b * nj + j])
            return tuple(acc)

        zero = tuple(jnp.zeros((SUB, LANES), jnp.float32) for _ in range(6 * nj))
        acc = pick(my_col, lambda n: vv[k, n : n + 1, :], zero)

        def one_peer(i, acc):
            peer = xor_index(my_col, i, ncol)
            pltpu.make_async_remote_copy(
                src_ref=vv.at[k],
                dst_ref=tab.at[k, peer],
                send_sem=vs_sem.at[k, i],
                recv_sem=vr_sem.at[k, i],
                device_id=(my_row, peer),
                device_id_type=MESH,
            ).wait_recv()
            return pick(peer, lambda n: tab[k, peer, n : n + 1, :], acc)

        acc = lax.fori_loop(1, ncol, one_peer, acc)
        halves = nrow // 2
        both = None
        for j in range(nj):
            for a in range(6):
                term = None
                for b in range(6):
                    product = b3[6 * a + b, j * SUB : (j + 1) * SUB, :] * acc[b * nj + j]
                    term = product if term is None else term + product
                tbuf[a * nchunk + j * SUB : a * nchunk + (j + 1) * SUB, :] = jnp.where(
                    slot_id + j * SUB * LANES < live_count, term, 0.0
                )
            for c in range(j * SUB, (j + 1) * SUB):
                here = jnp.broadcast_to(key[c : c + 1, :], (SUB, LANES)) - sub_q
                stacked = []
                for p in range(pairs):
                    first = p * per * nchunk + c
                    value = jnp.broadcast_to(tbuf[first : first + 1, :], (SUB, LANES))
                    for o in range(1, per):
                        n = (p * per + o) * nchunk + c
                        other = jnp.broadcast_to(tbuf[n : n + 1, :], (SUB, LANES))
                        value = jnp.where(sub_b == o, other, value)
                    stacked.append(value)
                rows = []
                for d in range(halves):
                    chosen = here == d * qn
                    for p in range(pairs):
                        rows.append(jnp.where(chosen, stacked[p], 0.0))
                full = jnp.concatenate(rows, axis=0)
                upper = full.astype(jnp.bfloat16)
                rest = (full - upper.astype(jnp.float32)).astype(jnp.bfloat16)
                spread[0 : halves * vec, c * LANES : (c + 1) * LANES] = upper
                spread[halves * vec : 2 * halves * vec, c * LANES : (c + 1) * LANES] = rest
            span = slice(j * SUB * LANES, (j + 1) * SUB * LANES)
            product = lax.dot_general(
                spread[:, span], onehot[:, span], (((1,), (1,)), ((), ())),
                preferred_element_type=jnp.float32,
            )
            both = product if both is None else both + product
        total = both[: halves * vec] + both[halves * vec :]
        for d in range(nrow):
            h, o = d // 2, d % 2
            part[k, d, 0:vec, :] = total[h * vec : (h + 1) * vec, o * LANES : (o + 1) * LANES]

    def send_parts(k):
        size = msg if k == ITERS - 1 else vec
        copies = []
        for i in range(1, nrow):
            peer = xor_index(my_row, i, nrow)
            copy = pltpu.make_async_remote_copy(
                src_ref=part.at[k, peer, pl.ds(0, size)],
                dst_ref=rbuf.at[k, my_row, pl.ds(0, size)],
                send_sem=ps_sem.at[k, i],
                recv_sem=pr_sem.at[k, i],
                device_id=(peer, my_col),
                device_id_type=MESH,
            )
            copy.start()
            copies.append(copy)
        return copies

    def diag_image(k):
        out = []
        v = [vv[k, b * qn : (b + 1) * qn, :] for b in range(6)]
        for a in range(6):
            value = diag(6 * a) * v[0]
            for b in range(1, 6):
                value = value + diag(6 * a + b) * v[b]
            out.append(value)
        return out

    def row_sum(value):
        return jnp.sum(value, axis=0, keepdims=True)

    moments = [row_sum(vv[0] * rv[0])]
    for k in range(ITERS):
        own = diag_image(k)
        for a in range(6):
            rv[k + 1, a * qn : (a + 1) * qn, :] = rv[k, a * qn : (a + 1) * qn, :] - own[a]
        if k == ITERS - 1:
            curv = 0.0
            for a in range(6):
                curv = curv + row_sum(vv[k, a * qn : (a + 1) * qn, :] * own[a])
        tile_partial(k)
        if k == ITERS - 1:
            curv = curv + row_sum(vv[k] * part[k, my_row, 0:vec, :])
            for i in range(1, nrow):
                peer = xor_index(my_row, i, nrow)
                row_copies[i - 1].wait_recv()
                curv = curv + row_sum(vrow[peer] * part[k, peer, 0:vec, :])
            moments.append(curv)
            packed = jnp.zeros((SUB, LANES), jnp.float32)
            for n, value in enumerate(moments):
                packed = jnp.where(sub == n, jnp.sum(value, axis=1, keepdims=True), packed)
            for d in range(nrow):
                part[k, d, vec:msg, :] = packed
        sent = send_parts(k)
        image = part[k, my_row, 0:vec, :]
        for i in range(1, nrow):
            sent[i - 1].wait_recv()
            peer = xor_index(my_row, i, nrow)
            image = image + rbuf[k, peer, 0:vec, :]
            if k == ITERS - 1:
                packed = packed + rbuf[k, peer, vec:msg, :]
        sends += sent
        if k == ITERS - 1:
            mown[...] = packed
            total_m = packed
            mom_sends = []
            for i in range(1, ncol):
                copy = pltpu.make_async_remote_copy(
                    src_ref=mown,
                    dst_ref=mom.at[my_col],
                    send_sem=ms_sem.at[i],
                    recv_sem=mr_sem.at[i],
                    device_id=(my_row, xor_index(my_col, i, ncol)),
                    device_id_type=MESH,
                )
                copy.start()
                mom_sends.append(copy)
        rv[k + 1] = rv[k + 1] - image
        if k + 1 < ITERS:
            precondition(k + 1)
            sends += send_vector(k + 1)
            if k + 1 == ITERS - 1:
                row_copies = send_rows(k + 1)
            moments.append(row_sum(vv[k] * rv[k + 1]))
            moments.append(row_sum(vv[k + 1] * rv[k + 1]))

    for i in range(1, ncol):
        mom_sends[i - 1].wait_recv()
        total_m = total_m + mom[xor_index(my_col, i, ncol)]
    m = [total_m[n : n + 1, :] for n in range(2 * ITERS)]
    m[2 * ITERS - 1] = m[2 * ITERS - 2] - m[2 * ITERS - 1]
    xc, rc = cg_scalars(m)
    for b in range(6):
        for q in range(qn):
            n = b * qn + q
            x = None
            r = None
            for k in range(ITERS + 1):
                add = rc[k] * rv[k, n : n + 1, :]
                r = add if r is None else r + add
                if k < ITERS:
                    add = xc[k] * vv[k, n : n + 1, :]
                    x = add if x is None else x + add
            x_ref[b : b + 1, q * LANES : (q + 1) * LANES] = x
            r_ref[b : b + 1, q * LANES : (q + 1) * LANES] = r
    for copy in sends + row_copies + mom_sends:
        copy.wait_send()


def on_device(nrow, ncol, minus_gradient, diag_blocks, hess_blocks, block_rows, block_cols, counts):
    pose_dev = minus_gradient.shape[1]
    nslot = block_rows.shape[-1]
    nchunk = nslot // LANES
    vec = 6 * pose_dev // LANES
    msg = vec + SUB
    f32 = jnp.float32
    vmem = pl.BlockSpec(memory_space=pltpu.VMEM)
    dma = pltpu.SemaphoreType.DMA
    out = jax.ShapeDtypeStruct(minus_gradient.shape, f32)
    return pl.pallas_call(
        functools.partial(kernel, nrow, ncol),
        out_shape=(out, out),
        in_specs=[
            pl.BlockSpec(memory_space=pltpu.HBM) for _ in range(6)
        ],
        out_specs=(vmem, vmem),
        scratch_shapes=[
            pltpu.SMEM((1, 1), jnp.int32),
            pltpu.VMEM(minus_gradient.shape, f32),
            pltpu.VMEM(diag_blocks.shape, f32),
            pltpu.VMEM((nchunk, LANES), jnp.int32),
            pltpu.VMEM((nchunk, LANES), jnp.int32),
            pltpu.VMEM((36, nchunk, LANES), f32),
            pltpu.VMEM((6 * vec, LANES), f32),
            pltpu.VMEM((21, pose_dev // LANES, LANES), f32),
            pltpu.VMEM((ITERS + 1, vec, LANES), f32),
            pltpu.VMEM((ITERS, vec, LANES), f32),
            pltpu.VMEM((ITERS, ncol, vec, LANES), f32),
            pltpu.VMEM((nrow, vec, LANES), f32),
            pltpu.VMEM((nchunk, LANES), jnp.int32),
            pltpu.VMEM((6 * nchunk, LANES), f32),
            pltpu.VMEM((nrow * vec, nslot), jnp.bfloat16),
            pltpu.VMEM((2 * LANES, nslot), jnp.bfloat16),
            pltpu.VMEM((ITERS, nrow, msg, LANES), f32),
            pltpu.VMEM((ITERS, nrow, msg, LANES), f32),
            pltpu.VMEM((ncol, SUB, LANES), f32),
            pltpu.VMEM((SUB, LANES), f32),
            dma((6,)),
            dma((ITERS, ncol)), dma((ITERS, ncol)),
            dma((nrow,)), dma((nrow,)),
            dma((ITERS, nrow)), dma((ITERS, nrow)),
            dma((ncol,)), dma((ncol,)),
        ],
        compiler_params=pltpu.CompilerParams(
            collective_id=0, has_side_effects=True, vmem_limit_bytes=67043328 - 64 * 1024
        ),
    )(
        counts,
        minus_gradient,
        diag_blocks,
        block_rows.reshape(nchunk, LANES),
        block_cols.reshape(nchunk, LANES),
        hess_blocks.reshape(36, nchunk, LANES),
    )


def solution(mesh):
    placed = (
        P(None, ("row", "col")),
        P(None, ("row", "col")),
        P("row", "col", None, None),
        P("row", "col", None),
        P("row", "col", None),
        P("row", "col"),
    )
    return jax.shard_map(
        functools.partial(on_device, mesh.shape["row"], mesh.shape["col"]),
        mesh=mesh,
        in_specs=placed,
        out_specs=(P(None, ("row", "col")), P(None, ("row", "col"))),
        check_vma=False,
    )
```
